32 devices in a mesh: tm: 8 (over z, x), space: 4 (over y, core).
Axes of the slice: x: 2, y: 2, z: 4, core: 2. Of those that a mesh axis runs over, the one named last changes fastest.
Arguments:
- forcing: bfloat16 [128, 256, 256], P('tm', 'space'), may hold values from -0.59765625 to 0.59765625
- starting_heat: bfloat16 [256, 256], P('space'), may hold values from -3 to 3, as said below
Outputs:
- heat_history: float32 [128, 256, 256], P('tm', 'space')
- history: float32 [2, 32], P(None, 'tm')
- change: float32 [2, 32], P(None, 'tm')
The draws below stay inside these ranges and needn't reach their ends.
Inputs may be any that keep to these rules, and one draw needn't show every extreme that they name: starting_heat is a combination of the 64 sine modes with both indices from 1 to 8, scaled so that its largest magnitude is 3.
All inputs are finite; a program needn't handle non-finite values.
Results may differ from the reference program's by a relative error of at most 0.0016.
Values may be sent and summed in bfloat16 or wider, within the bound.
A program may use at most 64 MiB of HBM per device.

```python
import math
import jax
import jax.numpy as jnp
from jax import lax

GRID = 256
FINE_FACTOR = 4
COARSE_FACTOR = 4
ITERS = 2
NT = 128
C_POINTS = 32
TOP_POINTS = 8


def draw_starting_heat(key, part):
    mode_index = jnp.arange(1, 9, dtype=jnp.int32)
    cell_index = jnp.arange(1, GRID + 1, dtype=jnp.int32)
    product = mode_index[:, None] * cell_index[None, :] % (2 * (GRID + 1))
    sine_rows = jnp.sin(jnp.pi * product.astype(jnp.float32) / (GRID + 1))
    weights = jax.random.normal(key, (8, 8), jnp.float32)
    inner = jnp.dot(weights, sine_rows, precision=lax.Precision.HIGHEST)
    summed = jnp.dot(sine_rows.T, inner, precision=lax.Precision.HIGHEST)
    scaled = 3.0 * summed / jnp.max(jnp.abs(summed))
    return scaled.astype(jnp.bfloat16)


def block_scale(rng, dims, cuts, low, top_value):
    gain = 1.0
    for axis_at, parts in cuts:
        draws = jax.random.uniform(jax.random.fold_in(jax.random.fold_in(rng, 6), axis_at), (parts,), jnp.float32, low / len(cuts), top_value / len(cuts))
        gain = gain * jnp.repeat(jnp.exp(draws), dims[axis_at] // parts).reshape((-1,) + (1,) * (len(dims) - 1 - axis_at))
    return gain


def bell_draw(stream_key, extent, spread, reach, shards=(), kind=jnp.bfloat16):
    level = block_scale(stream_key, extent, shards, -0.22, 0.18) if shards else 1.0
    result = jax.random.normal(stream_key, extent, jnp.float32) * spread * level
    return jnp.minimum(jnp.maximum(result, -reach), reach).astype(kind)


def setup_inputs(seed: int = 0) -> dict:
    keys = jax.random.split(jax.random.key(seed), 3)
    forcing = bell_draw(keys[0], (NT, GRID, GRID), 0.1, 0.59765625, ((0, 8), (1, 4)))
    starting_heat = draw_starting_heat(jax.random.fold_in(keys[2], 71), 0)
    return dict(forcing=forcing, starting_heat=starting_heat)


DURATION = 0.004

def sine_table(sample_locations, number_type):
    numbers = jnp.arange(1, sample_locations + 1, dtype=jnp.int32)
    product = numbers[:, None] * numbers[None, :] % (2 * (sample_locations + 1))
    angles = jnp.pi * product.astype(jnp.float32) / (sample_locations + 1)
    return (math.sqrt(2.0 / (sample_locations + 1)) * jnp.sin(angles)).astype(number_type)

def eigenvalues(sample_locations, first_mode, mode_count):
    numbers = (first_mode + jnp.arange(mode_count, dtype=jnp.int32) + 1).astype(jnp.float32)
    halves = jnp.sin(jnp.pi * numbers / (2 * (sample_locations + 1)))
    return 4.0 * (sample_locations + 1) ** 2 * halves * halves

def smoothing_pass(starts, sources, factor):
    current = starts
    visited = []
    for column in range(sources.shape[1] - 1):
        current = factor * current + sources[:, column]
        visited.append(current)
    return visited

def forward_block(field_block, table_half):
    halved = jnp.dot(field_block.reshape(-1, GRID), table_half, preferred_element_type=jnp.float32)
    halved = lax.optimization_barrier(halved.astype(jnp.bfloat16).reshape(field_block.shape))
    return jnp.einsum('xi,tiy->txy', table_half.astype(jnp.float32), halved.astype(jnp.float32), precision=lax.Precision.HIGHEST)

def reference(forcing, starting_heat):
    table_half = sine_table(GRID, jnp.bfloat16)
    table_full = sine_table(GRID, jnp.float32)
    decay_rates = eigenvalues(GRID, 0, GRID)[:, None] + eigenvalues(GRID, 0, GRID)[None, :]
    increment_duration = DURATION / NT
    per_increment_factor = 1.0 / (1.0 + increment_duration * decay_rates)
    mid_gain = 1.0 / (1.0 + FINE_FACTOR * increment_duration * decay_rates)
    top_gain = 1.0 / (1.0 + FINE_FACTOR * COARSE_FACTOR * increment_duration * decay_rates)
    start_field = forward_block(starting_heat[None], table_half)[0]

    def source_block(field_block):
        return per_increment_factor * forward_block(field_block, table_half)
    grouped = forcing.reshape(C_POINTS, FINE_FACTOR, GRID, GRID)
    sources = lax.map(source_block, grouped)
    values = jnp.zeros((C_POINTS, GRID, GRID), jnp.float32)
    history_rows = []
    change_rows = []
    for iteration in range(ITERS):
        begins = jnp.concatenate([start_field[None], values[:-1]], 0)
        ends_one = smoothing_pass(begins, sources, per_increment_factor)[-1]
        relaxed = per_increment_factor * ends_one + sources[:, -1]
        ends_two = smoothing_pass(jnp.concatenate([start_field[None], relaxed[:-1]], 0), sources, per_increment_factor)[-1]
        residual = sources[:, -1] + per_increment_factor * ends_two - relaxed
        history_rows.append(jnp.sqrt(lax.optimization_barrier(jnp.sum(residual * residual, axis=(1, 2))) / (GRID * GRID)))
        coarse_rhs = residual.reshape(TOP_POINTS, COARSE_FACTOR, GRID, GRID)
        running = coarse_rhs[:, 0]
        for column in range(1, COARSE_FACTOR):
            running = mid_gain * running + coarse_rhs[:, column]

        def advance(carried, source):
            updated = top_gain * carried + source
            return (updated, updated)
        unused, coarse_values = lax.scan(advance, jnp.zeros((GRID, GRID), jnp.float32), running)
        begins = jnp.concatenate([jnp.zeros((1, GRID, GRID), jnp.float32), coarse_values[:-1]], 0)
        pieces = smoothing_pass(begins, coarse_rhs, mid_gain)
        correction = jnp.stack(pieces + [coarse_values], axis=1).reshape(C_POINTS, GRID, GRID)
        values = relaxed + correction
        corr_sq = lax.optimization_barrier(jnp.sum(correction * correction, axis=(1, 2)))
        value_sq = lax.optimization_barrier(jnp.sum(values * values, axis=(1, 2)))
        change_rows.append(jnp.sqrt(corr_sq / value_sq))
    starts = jnp.concatenate([start_field[None], values[:-1]], 0)

    def finish(items):
        begin_value, block_sources, end_value = items
        inside = smoothing_pass(begin_value[None], block_sources[None], per_increment_factor)
        spectral_path = jnp.concatenate([jnp.stack(inside, axis=1)[0], end_value[None]], 0)
        rows_back = jnp.einsum('xi,tiy->txy', table_full, spectral_path, precision=lax.Precision.HIGHEST)
        rows_back = lax.optimization_barrier(rows_back.astype(jnp.bfloat16))
        return jnp.einsum('txi,iy->txy', rows_back.astype(jnp.float32), table_half.astype(jnp.float32), precision=lax.Precision.HIGHEST)
    heat_history = lax.map(finish, (starts, sources, values)).reshape(NT, GRID, GRID)
    return (heat_history, jnp.stack(history_rows), jnp.stack(change_rows))
```

```python
import functools
import math

import jax
import jax.numpy as jnp
import numpy as np
from jax import lax
from jax.experimental import pallas as pl
from jax.experimental.pallas import tpu as pltpu
from jax.sharding import PartitionSpec as P

FINE_FACTOR = 4
COARSE_FACTOR = 4
ITERS = 2
DURATION = 0.004
LANES = 128
MESH = pl.DeviceIdType.MESH
F32 = jnp.float32
BF16 = jnp.bfloat16


def sine_table(size):
    numbers = np.arange(1, size + 1, dtype=np.int64)
    product = numbers[:, None] * numbers[None, :] % (2 * (size + 1))
    return (math.sqrt(2.0 / (size + 1)) * np.sin(np.pi * product / (size + 1))).astype(np.float32)


def eigenvalues(size):
    numbers = np.arange(1, size + 1, dtype=np.float64)
    return 4.0 * (size + 1) ** 2 * np.sin(np.pi * numbers / (2 * (size + 1))) ** 2


def tables(size, slabs):
    width = size // slabs
    full = sine_table(size)
    half = full.astype(BF16)
    low = (full - half.astype(np.float32)).astype(BF16)
    back = np.zeros((slabs, 2, width, 2, size), BF16)
    for part in range(2):
        back[:, part, :, part, :] = half.reshape(slabs, width, size)
    back = back.reshape(2 * size, 2 * size)
    mu = eigenvalues(size)
    rate = mu.reshape(1, 2, size // 2, 1) + mu.reshape(slabs, 1, 1, width)
    rate = rate.transpose(0, 2, 1, 3).reshape(slabs, size // 2, 2 * width).astype(np.float32)
    return half, low, back, rate


def swap(low, a, b):
    half = LANES // 2
    return (
        jnp.where(low, a, pltpu.roll(b, half, 1)),
        jnp.where(low, pltpu.roll(a, half, 1), b),
    )


def kernel(n_tm, n_sp, rounds, f_ref, s_ref, half_ref, low_ref, back_ref, rate_ref,
           out_ref, hist_ref, chg_ref,
           sbuf, rbuf, src, path, tbuf, ubuf, lbuf, gbuf, zbuf, lrx, grx, zrx, vref, aref, stats, srx,
           f_send, f_recv, f_local, b_send, b_recv, b_local, t_send, t_recv, q_send, q_recv):
    tm, sp = lax.axis_index("tm"), lax.axis_index("space")
    steps, rows, size = f_ref.shape
    pairs = steps // 2
    inner = size // 2
    first = tm == 0
    distances = [1, 2] + [d for d in rounds if d > 2]
    peers = [lax.rem(sp + k, n_sp) for k in range(n_sp)]
    low = lax.broadcasted_iota(jnp.int32, (1, LANES), 1) < LANES // 2

    barrier = pltpu.get_barrier_semaphore()
    count = n_sp - 1
    for k in range(1, n_sp):
        pl.semaphore_signal(barrier, inc=1, device_id={"space": peers[k]}, device_id_type=MESH)
    for d in distances:
        @pl.when(tm + d < n_tm)
        def _():
            pl.semaphore_signal(barrier, inc=1, device_id={"tm": tm + d}, device_id_type=MESH)

        @pl.when(tm >= d)
        def _():
            pl.semaphore_signal(barrier, inc=1, device_id={"tm": tm - d}, device_id_type=MESH)
        count = count + (tm + d < n_tm).astype(jnp.int32) + (tm >= d).astype(jnp.int32)

    groups = [(p, p + 2) for p in range(0, pairs, 2)]
    groups[0] = (0, 2)
    f_groups = [(pairs, pairs + 1)] + groups

    def exchange(source, target, lo, hi, index, send, recv, local):
        copies = []
        for k in range(1, n_sp):
            copies.append(pltpu.make_async_remote_copy(
                src_ref=source.at[peers[k], pl.ds(lo, hi - lo)],
                dst_ref=target.at[sp, pl.ds(lo, hi - lo)],
                send_sem=send.at[index, k], recv_sem=recv.at[index, k],
                device_id={"space": peers[k]}, device_id_type=MESH))
        copies.append(pltpu.make_async_copy(
            source.at[sp, pl.ds(lo, hi - lo)], target.at[sp, pl.ds(lo, hi - lo)], local.at[index]))
        return copies

    forward = []
    for index, (lo, hi) in enumerate(f_groups):
        if lo == pairs:
            a = jnp.dot(s_ref[...], half_ref[...], preferred_element_type=F32)
            b = a
        else:
            a = jnp.dot(f_ref[lo:hi].reshape((hi - lo) * rows, size), half_ref[...],
                        preferred_element_type=F32)
            b = jnp.dot(f_ref[pairs + lo:pairs + hi].reshape((hi - lo) * rows, size), half_ref[...],
                        preferred_element_type=F32)
        for g in range(size // LANES):
            window = slice(g * LANES, (g + 1) * LANES)
            even, odd = swap(low, a[:, window], b[:, window])
            sbuf[2 * g, lo:hi] = even.astype(BF16).reshape(hi - lo, rows, LANES)
            sbuf[2 * g + 1, lo:hi] = odd.astype(BF16).reshape(hi - lo, rows, LANES)
        if index == 0:
            pl.semaphore_wait(barrier, count)
        copies = exchange(sbuf, rbuf, lo, hi, index, f_send, f_recv, f_local)
        for copy in copies:
            copy.start()
        forward.append(copies)

    step = DURATION / (steps * n_tm)
    rate = rate_ref[sp]
    gain = 1.0 / (1.0 + step * rate)
    mid = 1.0 / (1.0 + FINE_FACTOR * step * rate)
    top = 1.0 / (1.0 + FINE_FACTOR * COARSE_FACTOR * step * rate)
    gain4 = (gain * gain) * (gain * gain)
    mid2 = mid * mid
    push = mid2 * mid * gain4
    ratio = push / top

    begin = None
    for index, (lo, hi) in enumerate(f_groups):
        for copy in forward[index][:-1]:
            copy.wait_recv()
        forward[index][-1].wait()
        block = jnp.concatenate(
            [rbuf[:, p].reshape(size, LANES) for p in range(lo, hi)], axis=1)
        spectra = jnp.dot(half_ref[...], block, preferred_element_type=F32)
        for q, p in enumerate(range(lo, hi)):
            window = slice(q * LANES, (q + 1) * LANES)
            one, two = swap(low, spectra[:inner, window], spectra[inner:, window])
            if p == pairs:
                begin = one
                path[0] = one
            else:
                src[p] = gain * one
                src[pairs + p] = gain * two

    for i in range(COARSE_FACTOR):
        total = src[FINE_FACTOR * i]
        for j in range(1, FINE_FACTOR):
            total = gain * total + src[FINE_FACTOR * i + j]
        tbuf[i] = total
    begin = path[0]

    vref[0] = jnp.where(first, begin, 0.0)
    for i in range(1, COARSE_FACTOR + 1):
        vref[i] = jnp.zeros_like(begin)

    sent = []

    def along(source, target, slot, it, distance):
        copy = pltpu.make_async_remote_copy(
            src_ref=source, dst_ref=target,
            send_sem=t_send.at[it, slot], recv_sem=t_recv.at[it, slot],
            device_id={"tm": tm + distance}, device_id_type=MESH)
        sent.append((copy, distance))

        @pl.when(tm + distance < n_tm)
        def _():
            copy.start()
        return copy

    for it in range(ITERS):
        last = COARSE_FACTOR - 1
        newest = gain4 * vref[last] + tbuf[last]
        lbuf[it] = newest
        shift = along(lbuf.at[it], lrx.at[it], 0, it, 1)
        relaxed = [gain4 * vref[i] + tbuf[i] for i in range(last)] + [newest]
        residual = [None] + [gain4 * (relaxed[i - 1] - vref[i]) for i in range(1, COARSE_FACTOR)]
        local = residual[1]
        for i in range(2, COARSE_FACTOR):
            local = mid * local + residual[i]
        gbuf[it] = local - jnp.where(first, 0.0, push * vref[0]) + ratio * newest
        near = along(gbuf.at[it], grx.at[it, 0], 1, it, 1)
        far = along(gbuf.at[it], grx.at[it, 1], 2, it, 2)
        for i in range(COARSE_FACTOR):
            ubuf[i] = relaxed[i]
        zbuf[it, 0] = jnp.zeros_like(begin)
        aref[...] = begin

        @pl.when(tm >= 1)
        def _():
            shift.wait_recv()
            aref[...] = lrx[it]
            near.wait_recv()
            zbuf[it, 0] = grx[it, 0]

        @pl.when(tm >= 2)
        def _():
            far.wait_recv()
            zbuf[it, 0] = zbuf[it, 0] + top * grx[it, 1]
        power = top * top
        for r, d in enumerate(rounds):
            copy = along(zbuf.at[it, r], zrx.at[it, r], 3 + r, it, d)
            zbuf[it, r + 1] = zbuf[it, r]

            @pl.when(tm >= d)
            def _():
                copy.wait_recv()
                zbuf[it, r + 1] = zbuf[it, r + 1] + power * zrx[it, r]
            power = power * power
        arrived = aref[...]
        incoming = jnp.where(first, 0.0, zbuf[it, len(rounds)] - ratio * arrived)
        before = vref[0]
        keep = incoming
        for i in range(COARSE_FACTOR):
            if i == 0:
                res = gain4 * (arrived - before)
                run = res
            else:
                res = gain4 * (ubuf[i - 1] - vref_old)
                run = mid * run + res
            vref_old = vref[i + 1]
            if i < COARSE_FACTOR - 1:
                keep = mid * keep + res
            else:
                keep = top * incoming + run
            value = ubuf[i] + keep
            vref[i + 1] = value
            for kind, item in enumerate((res, keep, value)):
                at = (kind * ITERS + it) * COARSE_FACTOR + i
                stats[at:at + 1] = jnp.sum(item * item, axis=0, keepdims=True)
        vref[0] = arrived + incoming

    tallies = []
    for k in range(1, n_sp):
        copy = pltpu.make_async_remote_copy(
            src_ref=stats, dst_ref=srx.at[sp], send_sem=q_send.at[k], recv_sem=q_recv.at[k],
            device_id={"space": peers[k]}, device_id_type=MESH)
        copy.start()
        tallies.append(copy)

    for i in range(COARSE_FACTOR):
        current = vref[i]
        for j in range(FINE_FACTOR - 1):
            current = gain * current + src[FINE_FACTOR * i + j]
            path[FINE_FACTOR * i + j] = current
        path[FINE_FACTOR * i + FINE_FACTOR - 1] = vref[i + 1]

    for copies in forward:
        for copy in copies[:-1]:
            copy.wait_send()
    backward = []
    for index, (lo, hi) in enumerate(groups):
        columns = []
        for p in range(lo, hi):
            upper, lower = swap(low, path[p], path[pairs + p])
            columns.append(jnp.concatenate([upper, lower], axis=0))
        block = jnp.concatenate(columns, axis=1)
        high = block.astype(BF16)
        rest = (block - high.astype(F32)).astype(BF16)
        back = jnp.dot(low_ref[...], high, preferred_element_type=F32)
        back = back + jnp.dot(half_ref[...], rest, preferred_element_type=F32)
        back = back + jnp.dot(half_ref[...], high, preferred_element_type=F32)
        back = back.astype(BF16)
        for j in range(n_sp):
            for q, p in enumerate(range(lo, hi)):
                bsend_block = back[j * rows:(j + 1) * rows, q * LANES:(q + 1) * LANES]
                sbuf[j, pairs + 1 + p] = bsend_block
        copies = exchange(sbuf, rbuf, pairs + 1 + lo, pairs + 1 + hi, index, b_send, b_recv, b_local)
        for copy in copies:
            copy.start()
        backward.append(copies)

    for index, (lo, hi) in enumerate(groups):
        for copy in backward[index][:-1]:
            copy.wait_recv()
        backward[index][-1].wait()
        block = jnp.concatenate(
            [rbuf[j, pairs + 1 + lo:pairs + 1 + hi].reshape((hi - lo) * rows, LANES)
             for j in range(n_sp)], axis=1)
        heat = jnp.dot(block, back_ref[...], preferred_element_type=F32)
        out_ref[lo:hi] = heat[:, :size].reshape(hi - lo, rows, size)
        out_ref[pairs + lo:pairs + hi] = heat[:, size:].reshape(hi - lo, rows, size)

    total = stats[...]
    for k in range(1, n_sp):
        tallies[k - 1].wait_recv()
        total = total + srx[lax.rem(sp - k + n_sp, n_sp)]
    total = jnp.sum(total, axis=1, keepdims=True)
    points = ITERS * COARSE_FACTOR
    residual_norm = jnp.sqrt(total[:points] / (size * size))
    relative = jnp.sqrt(total[points:2 * points] / total[2 * points:3 * points])
    shape = (ITERS, COARSE_FACTOR)
    where = (lax.broadcasted_iota(jnp.int32, shape, 0) * COARSE_FACTOR
             + lax.broadcasted_iota(jnp.int32, shape, 1))
    hist = jnp.zeros(shape, F32)
    chg = jnp.zeros(shape, F32)
    for k in range(points):
        hist = jnp.where(where == k, residual_norm[k:k + 1], hist)
        chg = jnp.where(where == k, relative[k:k + 1], chg)
    hist_ref[...] = hist
    chg_ref[...] = chg

    for copies in backward:
        for copy in copies[:-1]:
            copy.wait_send()
    for copy in tallies:
        copy.wait_send()
    for copy, distance in sent:
        @pl.when(tm + distance < n_tm)
        def _():
            copy.wait_send()


def shards(forcing, starting_heat):
    steps, rows, size = forcing.shape
    n_tm, n_sp = lax.axis_size("tm"), lax.axis_size("space")
    assert steps == FINE_FACTOR * COARSE_FACTOR and 2 * rows == LANES
    pairs = steps // 2
    rounds = []
    reach = 2
    while reach < n_tm - 1:
        rounds.append(reach)
        reach *= 2
    half, low, back, rate = tables(size, n_sp)
    state = (size // 2, LANES)
    slots = len(rounds) + 1
    chunks = pairs // 2 + 1
    stat_rows = 3 * ITERS * COARSE_FACTOR
    dma = pltpu.SemaphoreType.DMA
    vmem = pl.BlockSpec(memory_space=pltpu.VMEM)
    return pl.pallas_call(
        functools.partial(kernel, n_tm, n_sp, tuple(rounds)),
        out_shape=(
            jax.ShapeDtypeStruct((steps, rows, size), F32),
            jax.ShapeDtypeStruct((ITERS, COARSE_FACTOR), F32),
            jax.ShapeDtypeStruct((ITERS, COARSE_FACTOR), F32),
        ),
        in_specs=[vmem] * 6,
        out_specs=(vmem,) * 3,
        scratch_shapes=[
            pltpu.VMEM((n_sp, 2 * pairs + 1, rows, LANES), BF16),
            pltpu.VMEM((n_sp, 2 * pairs + 1, rows, LANES), BF16),
            pltpu.VMEM((steps,) + state, F32),
            pltpu.VMEM((steps,) + state, F32),
            pltpu.VMEM((COARSE_FACTOR,) + state, F32),
            pltpu.VMEM((COARSE_FACTOR,) + state, F32),
            pltpu.VMEM((ITERS,) + state, F32),
            pltpu.VMEM((ITERS,) + state, F32),
            pltpu.VMEM((ITERS, slots) + state, F32),
            pltpu.VMEM((ITERS,) + state, F32),
            pltpu.VMEM((ITERS, 2) + state, F32),
            pltpu.VMEM((ITERS, slots) + state, F32),
            pltpu.VMEM((COARSE_FACTOR + 1,) + state, F32),
            pltpu.VMEM(state, F32),
            pltpu.VMEM((stat_rows, LANES), F32),
            pltpu.VMEM((n_sp, stat_rows, LANES), F32),
            dma((chunks, n_sp)), dma((chunks, n_sp)), dma((chunks,)),
            dma((chunks, n_sp)), dma((chunks, n_sp)), dma((chunks,)),
            dma((ITERS, 3 + len(rounds))), dma((ITERS, 3 + len(rounds))),
            dma((n_sp,)), dma((n_sp,)),
        ],
        compiler_params=pltpu.CompilerParams(collective_id=0, has_side_effects=True),
    )(forcing, starting_heat, jnp.asarray(half), jnp.asarray(low), jnp.asarray(back),
      jnp.asarray(rate))


def solution(mesh):
    return jax.shard_map(
        shards,
        mesh=mesh,
        in_specs=(P("tm", "space", None), P("space", None)),
        out_specs=(P("tm", "space", None), P(None, "tm"), P(None, "tm")),
        check_vma=False,
    )
```

```python
import functools
import math

import jax
import jax.numpy as jnp
import numpy as np
from jax import lax
from jax.experimental import pallas as pl
from jax.experimental.pallas import tpu as pltpu
from jax.sharding import PartitionSpec as P

FINE_FACTOR = 4
COARSE_FACTOR = 4
ITERS = 2
DURATION = 0.004
LANES = 128
MESH = pl.DeviceIdType.MESH
F32 = jnp.float32
BF16 = jnp.bfloat16


def sine_table(size):
    numbers = np.arange(1, size + 1, dtype=np.int64)
    product = numbers[:, None] * numbers[None, :] % (2 * (size + 1))
    return (math.sqrt(2.0 / (size + 1)) * np.sin(np.pi * product / (size + 1))).astype(np.float32)


def eigenvalues(size):
    numbers = np.arange(1, size + 1, dtype=np.float64)
    return 4.0 * (size + 1) ** 2 * np.sin(np.pi * numbers / (2 * (size + 1))) ** 2


def tables(size, slabs):
    width = size // slabs
    full = sine_table(size)
    half = full.astype(BF16)
    low = (full - half.astype(np.float32)).astype(BF16)
    back = np.zeros((slabs, 2, width, 2, size), BF16)
    for part in range(2):
        back[:, part, :, part, :] = half.reshape(slabs, width, size)
    back = back.reshape(2 * size, 2 * size)
    mu = eigenvalues(size)
    rate = mu.reshape(1, 2, size // 2, 1) + mu.reshape(slabs, 1, 1, width)
    rate = rate.transpose(0, 2, 1, 3).reshape(slabs, size // 2, 2 * width).astype(np.float32)
    return half, low, back, rate


def swap(low, a, b):
    half = LANES // 2
    return (
        jnp.where(low, a, pltpu.roll(b, half, 1)),
        jnp.where(low, pltpu.roll(a, half, 1), b),
    )


def kernel(n_tm, n_sp, rounds, f_ref, s_ref, half_ref, low_ref, back_ref, rate_ref,
           out_ref, hist_ref, chg_ref,
           sbuf, rbuf, src, path, tbuf, ubuf, gbuf, zbuf, lrx, wrx, grx, zrx, vref, aref, stats, srx,
           f_send, f_recv, f_local, b_send, b_recv, b_local, t_send, t_recv, q_send, q_recv):
    tm, sp = lax.axis_index("tm"), lax.axis_index("space")
    steps, rows, size = f_ref.shape
    pairs = steps // 2
    inner = size // 2
    first = tm == 0
    distances = [1, 2] + [d for d in rounds if d > 2]
    peers = [lax.rem(sp + k, n_sp) for k in range(n_sp)]
    low = lax.broadcasted_iota(jnp.int32, (1, LANES), 1) < LANES // 2

    barrier = pltpu.get_barrier_semaphore()
    count = n_sp - 1
    for k in range(1, n_sp):
        pl.semaphore_signal(barrier, inc=1, device_id={"space": peers[k]}, device_id_type=MESH)
    for d in distances:
        @pl.when(tm + d < n_tm)
        def _():
            pl.semaphore_signal(barrier, inc=1, device_id={"tm": tm + d}, device_id_type=MESH)

        @pl.when(tm >= d)
        def _():
            pl.semaphore_signal(barrier, inc=1, device_id={"tm": tm - d}, device_id_type=MESH)
        count = count + (tm + d < n_tm).astype(jnp.int32) + (tm >= d).astype(jnp.int32)

    groups = [(p, p + 2) for p in range(0, pairs, 2)]
    groups[0] = (0, 2)
    f_groups = [(pairs, pairs + 1)] + groups

    def exchange(source, target, lo, hi, index, send, recv, local):
        copies = []
        for k in range(1, n_sp):
            copies.append(pltpu.make_async_remote_copy(
                src_ref=source.at[peers[k], pl.ds(lo, hi - lo)],
                dst_ref=target.at[sp, pl.ds(lo, hi - lo)],
                send_sem=send.at[index, k], recv_sem=recv.at[index, k],
                device_id={"space": peers[k]}, device_id_type=MESH))
        copies.append(pltpu.make_async_copy(
            source.at[sp, pl.ds(lo, hi - lo)], target.at[sp, pl.ds(lo, hi - lo)], local.at[index]))
        return copies

    forward = []
    for index, (lo, hi) in enumerate(f_groups):
        if lo == pairs:
            a = jnp.dot(s_ref[...], half_ref[...], preferred_element_type=F32)
            b = a
        else:
            a = jnp.dot(f_ref[lo:hi].reshape((hi - lo) * rows, size), half_ref[...],
                        preferred_element_type=F32)
            b = jnp.dot(f_ref[pairs + lo:pairs + hi].reshape((hi - lo) * rows, size), half_ref[...],
                        preferred_element_type=F32)
        for g in range(size // LANES):
            window = slice(g * LANES, (g + 1) * LANES)
            even, odd = swap(low, a[:, window], b[:, window])
            sbuf[2 * g, lo:hi] = even.astype(BF16).reshape(hi - lo, rows, LANES)
            sbuf[2 * g + 1, lo:hi] = odd.astype(BF16).reshape(hi - lo, rows, LANES)
        if index == 0:
            pl.semaphore_wait(barrier, count)
        copies = exchange(sbuf, rbuf, lo, hi, index, f_send, f_recv, f_local)
        for copy in copies:
            copy.start()
        forward.append(copies)

    step = DURATION / (steps * n_tm)
    rate = rate_ref[sp]
    gain = 1.0 / (1.0 + step * rate)
    mid = 1.0 / (1.0 + FINE_FACTOR * step * rate)
    top = 1.0 / (1.0 + FINE_FACTOR * COARSE_FACTOR * step * rate)
    gain4 = (gain * gain) * (gain * gain)
    mid2 = mid * mid
    push = mid2 * mid * gain4
    ratio = push / top

    begin = None
    for index, (lo, hi) in enumerate(f_groups):
        for copy in forward[index][:-1]:
            copy.wait_recv()
        forward[index][-1].wait()
        block = jnp.concatenate(
            [rbuf[:, p].reshape(size, LANES) for p in range(lo, hi)], axis=1)
        spectra = jnp.dot(half_ref[...], block, preferred_element_type=F32)
        for q, p in enumerate(range(lo, hi)):
            window = slice(q * LANES, (q + 1) * LANES)
            one, two = swap(low, spectra[:inner, window], spectra[inner:, window])
            if p == pairs:
                begin = one
                path[0] = one
            else:
                src[p] = gain * one
                src[pairs + p] = gain * two

    for i in range(COARSE_FACTOR):
        total = src[FINE_FACTOR * i]
        for j in range(1, FINE_FACTOR):
            total = gain * total + src[FINE_FACTOR * i + j]
        tbuf[i] = total
    begin = path[0]

    vref[0] = jnp.where(first, begin, 0.0)
    for i in range(1, COARSE_FACTOR + 1):
        vref[i] = jnp.zeros_like(begin)

    sent = []

    def along(source, target, slot, distance):
        copy = pltpu.make_async_remote_copy(
            src_ref=source, dst_ref=target,
            send_sem=t_send.at[slot], recv_sem=t_recv.at[slot],
            device_id={"tm": tm + distance}, device_id_type=MESH)
        sent.append((copy, distance))

        @pl.when(tm + distance < n_tm)
        def _():
            copy.start()
        return copy

    last = COARSE_FACTOR - 1
    shift = along(tbuf.at[last], lrx, 0, 1)
    drift = gain4 - mid
    slope = 3.0 * gain4 * mid2 * drift + ratio * (push - top)
    aref[...] = begin

    @pl.when(tm >= 1)
    def _():
        shift.wait_recv()
        aref[...] = lrx[...]

    arrived = aref[...]
    ubuf[0] = tbuf[0] + jnp.where(first, gain4 * begin, 0.0)
    bare = jnp.where(first, 0.0, gain4 * arrived)
    base = tbuf[0] + gain4 * arrived
    local = jnp.zeros_like(begin)
    for i in range(1, last):
        relaxed = ubuf[0] if i == 1 else tbuf[i - 1]
        bare = mid * bare + gain4 * relaxed
        local = mid * local + gain4 * (gain4 * base - bare)
        base = tbuf[i] + bare
        ubuf[i] = tbuf[i]
    ubuf[last] = tbuf[last]
    rhs = mid * bare + gain4 * tbuf[last - 1]
    change = gain4 * base - rhs
    zbuf[0, 0] = rhs
    zbuf[0, 1] = local + ratio * change
    near = along(zbuf.at[0], grx.at[0], 1, 1)
    far = along(zbuf.at[0], grx.at[1], 2, 2)
    gbuf[...] = change + (1.0 - ratio) * rhs
    step_in = along(gbuf, wrx, 3, 1)
    zbuf[1] = jnp.zeros((2,) + begin.shape, F32)

    @pl.when(tm >= 1)
    def _():
        near.wait_recv()
        zbuf[1] = grx[0]

    @pl.when(tm >= 2)
    def _():
        far.wait_recv()
        zbuf[1, 0] = zbuf[1, 0] + top * grx[1, 0]
        zbuf[1, 1] = zbuf[1, 1] + top * grx[1, 1] + slope * grx[1, 0]
    slope = 2.0 * top * slope
    power = top * top
    for r, d in enumerate(rounds):
        copy = along(zbuf.at[r + 1], zrx.at[r], 4 + r, d)
        zbuf[r + 2] = zbuf[r + 1]

        @pl.when(tm >= d)
        def _():
            copy.wait_recv()
            zbuf[r + 2, 0] = zbuf[r + 2, 0] + power * zrx[r, 0]
            zbuf[r + 2, 1] = zbuf[r + 2, 1] + power * zrx[r, 1] + slope * zrx[r, 0]
        slope = 2.0 * power * slope
        power = power * power
    aref[...] = jnp.zeros_like(begin)

    @pl.when(tm >= 1)
    def _():
        step_in.wait_recv()
        aref[...] = wrx[...] - (1.0 - ratio) * zbuf[len(rounds) + 1, 0]

    for it in range(ITERS):
        before = vref[0]
        if it == 0:
            incoming = zbuf[len(rounds) + 1, 0]
            ahead = jnp.where(first, 0.0, arrived)
        else:
            ahead = aref[...]
            incoming = zbuf[len(rounds) + 1, 1] - ratio * ahead
            arrived = before + ahead
            for i in range(COARSE_FACTOR):
                ubuf[i] = gain4 * vref[i] + tbuf[i]
        keep = incoming
        for i in range(COARSE_FACTOR):
            if i == 0:
                res = gain4 * ahead
                run = res
            else:
                res = gain4 * (ubuf[i - 1] - vref_old)
                run = mid * run + res
            vref_old = vref[i + 1]
            if i < COARSE_FACTOR - 1:
                keep = mid * keep + res
            else:
                keep = top * incoming + run
            value = ubuf[i] + keep
            vref[i + 1] = value
            for kind, item in enumerate((res, keep, value)):
                at = (kind * ITERS + it) * COARSE_FACTOR + i
                stats[at:at + 1] = jnp.sum(item * item, axis=0, keepdims=True)
        vref[0] = arrived + incoming

    tallies = []
    for k in range(1, n_sp):
        copy = pltpu.make_async_remote_copy(
            src_ref=stats, dst_ref=srx.at[sp], send_sem=q_send.at[k], recv_sem=q_recv.at[k],
            device_id={"space": peers[k]}, device_id_type=MESH)
        copy.start()
        tallies.append(copy)

    for i in range(COARSE_FACTOR):
        current = vref[i]
        for j in range(FINE_FACTOR - 1):
            current = gain * current + src[FINE_FACTOR * i + j]
            path[FINE_FACTOR * i + j] = current
        path[FINE_FACTOR * i + FINE_FACTOR - 1] = vref[i + 1]

    for copies in forward:
        for copy in copies[:-1]:
            copy.wait_send()
    backward = []
    for index, (lo, hi) in enumerate(groups):
        columns = []
        for p in range(lo, hi):
            upper, lower = swap(low, path[p], path[pairs + p])
            columns.append(jnp.concatenate([upper, lower], axis=0))
        block = jnp.concatenate(columns, axis=1)
        high = block.astype(BF16)
        rest = (block - high.astype(F32)).astype(BF16)
        back = jnp.dot(low_ref[...], high, preferred_element_type=F32)
        back = back + jnp.dot(half_ref[...], rest, preferred_element_type=F32)
        back = back + jnp.dot(half_ref[...], high, preferred_element_type=F32)
        back = back.astype(BF16)
        for j in range(n_sp):
            for q, p in enumerate(range(lo, hi)):
                bsend_block = back[j * rows:(j + 1) * rows, q * LANES:(q + 1) * LANES]
                sbuf[j, pairs + 1 + p] = bsend_block
        copies = exchange(sbuf, rbuf, pairs + 1 + lo, pairs + 1 + hi, index, b_send, b_recv, b_local)
        for copy in copies:
            copy.start()
        backward.append(copies)

    for index, (lo, hi) in enumerate(groups):
        for copy in backward[index][:-1]:
            copy.wait_recv()
        backward[index][-1].wait()
        block = jnp.concatenate(
            [rbuf[j, pairs + 1 + lo:pairs + 1 + hi].reshape((hi - lo) * rows, LANES)
             for j in range(n_sp)], axis=1)
        heat = jnp.dot(block, back_ref[...], preferred_element_type=F32)
        out_ref[lo:hi] = heat[:, :size].reshape(hi - lo, rows, size)
        out_ref[pairs + lo:pairs + hi] = heat[:, size:].reshape(hi - lo, rows, size)

    total = stats[...]
    for k in range(1, n_sp):
        tallies[k - 1].wait_recv()
        total = total + srx[lax.rem(sp - k + n_sp, n_sp)]
    total = jnp.sum(total, axis=1, keepdims=True)
    points = ITERS * COARSE_FACTOR
    residual_norm = jnp.sqrt(total[:points] / (size * size))
    relative = jnp.sqrt(total[points:2 * points] / total[2 * points:3 * points])
    shape = (ITERS, COARSE_FACTOR)
    where = (lax.broadcasted_iota(jnp.int32, shape, 0) * COARSE_FACTOR
             + lax.broadcasted_iota(jnp.int32, shape, 1))
    hist = jnp.zeros(shape, F32)
    chg = jnp.zeros(shape, F32)
    for k in range(points):
        hist = jnp.where(where == k, residual_norm[k:k + 1], hist)
        chg = jnp.where(where == k, relative[k:k + 1], chg)
    hist_ref[...] = hist
    chg_ref[...] = chg

    for copies in backward:
        for copy in copies[:-1]:
            copy.wait_send()
    for copy in tallies:
        copy.wait_send()
    for copy, distance in sent:
        @pl.when(tm + distance < n_tm)
        def _():
            copy.wait_send()


def shards(forcing, starting_heat):
    steps, rows, size = forcing.shape
    n_tm, n_sp = lax.axis_size("tm"), lax.axis_size("space")
    assert steps == FINE_FACTOR * COARSE_FACTOR and 2 * rows == LANES
    pairs = steps // 2
    rounds = []
    reach = 2
    while reach < n_tm - 1:
        rounds.append(reach)
        reach *= 2
    half, low, back, rate = tables(size, n_sp)
    state = (size // 2, LANES)
    slots = len(rounds) + 1
    chunks = pairs // 2 + 1
    stat_rows = 3 * ITERS * COARSE_FACTOR
    dma = pltpu.SemaphoreType.DMA
    vmem = pl.BlockSpec(memory_space=pltpu.VMEM)
    return pl.pallas_call(
        functools.partial(kernel, n_tm, n_sp, tuple(rounds)),
        out_shape=(
            jax.ShapeDtypeStruct((steps, rows, size), F32),
            jax.ShapeDtypeStruct((ITERS, COARSE_FACTOR), F32),
            jax.ShapeDtypeStruct((ITERS, COARSE_FACTOR), F32),
        ),
        in_specs=[vmem] * 6,
        out_specs=(vmem,) * 3,
        scratch_shapes=[
            pltpu.VMEM((n_sp, 2 * pairs + 1, rows, LANES), BF16),
            pltpu.VMEM((n_sp, 2 * pairs + 1, rows, LANES), BF16),
            pltpu.VMEM((steps,) + state, F32),
            pltpu.VMEM((steps,) + state, F32),
            pltpu.VMEM((COARSE_FACTOR,) + state, F32),
            pltpu.VMEM((COARSE_FACTOR,) + state, F32),
            pltpu.VMEM(state, F32),
            pltpu.VMEM((slots + 1, ITERS) + state, F32),
            pltpu.VMEM(state, F32),
            pltpu.VMEM(state, F32),
            pltpu.VMEM((2, ITERS) + state, F32),
            pltpu.VMEM((slots, ITERS) + state, F32),
            pltpu.VMEM((COARSE_FACTOR + 1,) + state, F32),
            pltpu.VMEM(state, F32),
            pltpu.VMEM((stat_rows, LANES), F32),
            pltpu.VMEM((n_sp, stat_rows, LANES), F32),
            dma((chunks, n_sp)), dma((chunks, n_sp)), dma((chunks,)),
            dma((chunks, n_sp)), dma((chunks, n_sp)), dma((chunks,)),
            dma((4 + len(rounds),)), dma((4 + len(rounds),)),
            dma((n_sp,)), dma((n_sp,)),
        ],
        compiler_params=pltpu.CompilerParams(collective_id=0, has_side_effects=True),
    )(forcing, starting_heat, jnp.asarray(half), jnp.asarray(low), jnp.asarray(back),
      jnp.asarray(rate))


def solution(mesh):
    return jax.shard_map(
        shards,
        mesh=mesh,
        in_specs=(P("tm", "space", None), P("space", None)),
        out_specs=(P("tm", "space", None), P(None, "tm"), P(None, "tm")),
        check_vma=False,
    )
```

```python
import functools
import math

import jax
import jax.numpy as jnp
import numpy as np
from jax import lax
from jax.experimental import pallas as pl
from jax.experimental.pallas import tpu as pltpu
from jax.sharding import PartitionSpec as P

FINE_FACTOR = 4
COARSE_FACTOR = 4
ITERS = 2
DURATION = 0.004
LANES = 128
MESH = pl.DeviceIdType.MESH
F32 = jnp.float32
BF16 = jnp.bfloat16


def sine_table(size):
    numbers = np.arange(1, size + 1, dtype=np.int64)
    product = numbers[:, None] * numbers[None, :] % (2 * (size + 1))
    return (math.sqrt(2.0 / (size + 1)) * np.sin(np.pi * product / (size + 1))).astype(np.float32)


def eigenvalues(size):
    numbers = np.arange(1, size + 1, dtype=np.float64)
    return 4.0 * (size + 1) ** 2 * np.sin(np.pi * numbers / (2 * (size + 1))) ** 2


def tables(size, slabs):
    width = size // slabs
    full = sine_table(size)
    half = full.astype(BF16)
    low = (full - half.astype(np.float32)).astype(BF16)
    back = np.zeros((slabs, 2, width, 2, size), BF16)
    for part in range(2):
        back[:, part, :, part, :] = half.reshape(slabs, width, size)
    back = back.reshape(2 * size, 2 * size)
    mu = eigenvalues(size)
    rate = mu.reshape(1, 2, size // 2, 1) + mu.reshape(slabs, 1, 1, width)
    rate = rate.transpose(0, 2, 1, 3).reshape(slabs, size // 2, 2 * width).astype(np.float32)
    return half, low, back, rate


def swap(low, a, b):
    half = LANES // 2
    return (
        jnp.where(low, a, pltpu.roll(b, half, 1)),
        jnp.where(low, pltpu.roll(a, half, 1), b),
    )


def kernel(n_tm, n_sp, rounds, f_ref, s_ref, half_ref, low_ref, rate_ref,
           out_ref, total_ref,
           sbuf, rbuf, src, path, tbuf, ubuf, gbuf, zbuf, lrx, wrx, grx, zrx, vref, aref, stats, srx,
           f_send, f_recv, f_local, b_send, b_recv, b_local, t_send, t_recv, q_send, q_recv):
    tm, sp = lax.axis_index("tm"), lax.axis_index("space")
    steps, rows, size = f_ref.shape
    pairs = steps // 2
    inner = size // 2
    first = tm == 0
    distances = [1, 2] + [d for d in rounds if d > 2]
    peers = [lax.rem(sp + k, n_sp) for k in range(n_sp)]
    low = lax.broadcasted_iota(jnp.int32, (1, LANES), 1) < LANES // 2

    barrier = pltpu.get_barrier_semaphore()
    count = n_sp - 1
    for k in range(1, n_sp):
        pl.semaphore_signal(barrier, inc=1, device_id={"space": peers[k]}, device_id_type=MESH)
    for d in distances:
        @pl.when(tm + d < n_tm)
        def _():
            pl.semaphore_signal(barrier, inc=1, device_id={"tm": tm + d}, device_id_type=MESH)

        @pl.when(tm >= d)
        def _():
            pl.semaphore_signal(barrier, inc=1, device_id={"tm": tm - d}, device_id_type=MESH)
        count = count + (tm + d < n_tm).astype(jnp.int32) + (tm >= d).astype(jnp.int32)

    groups = [(p, p + 2) for p in range(0, pairs, 2)]
    groups[0] = (0, 2)
    f_groups = [(pairs, pairs + 1)] + groups

    def exchange(source, target, lo, hi, index, send, recv, local):
        copies = []
        for k in range(1, n_sp):
            copies.append(pltpu.make_async_remote_copy(
                src_ref=source.at[peers[k], pl.ds(lo, hi - lo)],
                dst_ref=target.at[sp, pl.ds(lo, hi - lo)],
                send_sem=send.at[index, k], recv_sem=recv.at[index, k],
                device_id={"space": peers[k]}, device_id_type=MESH))
        copies.append(pltpu.make_async_copy(
            source.at[sp, pl.ds(lo, hi - lo)], target.at[sp, pl.ds(lo, hi - lo)], local.at[index]))
        return copies

    forward = []
    for index, (lo, hi) in enumerate(f_groups):
        if lo == pairs:
            a = jnp.dot(s_ref[...], half_ref[...], preferred_element_type=F32)
            b = a
        else:
            a = jnp.dot(f_ref[lo:hi].reshape((hi - lo) * rows, size), half_ref[...],
                        preferred_element_type=F32)
            b = jnp.dot(f_ref[pairs + lo:pairs + hi].reshape((hi - lo) * rows, size), half_ref[...],
                        preferred_element_type=F32)
        for g in range(size // LANES):
            window = slice(g * LANES, (g + 1) * LANES)
            even, odd = swap(low, a[:, window], b[:, window])
            sbuf[2 * g, lo:hi] = even.astype(BF16).reshape(hi - lo, rows, LANES)
            sbuf[2 * g + 1, lo:hi] = odd.astype(BF16).reshape(hi - lo, rows, LANES)
        if index == 0:
            pl.semaphore_wait(barrier, count)
        copies = exchange(sbuf, rbuf, lo, hi, index, f_send, f_recv, f_local)
        for copy in copies:
            copy.start()
        forward.append(copies)

    step = DURATION / (steps * n_tm)
    rate = rate_ref[sp]
    gain = 1.0 / (1.0 + step * rate)
    mid = 1.0 / (1.0 + FINE_FACTOR * step * rate)
    top = 1.0 / (1.0 + FINE_FACTOR * COARSE_FACTOR * step * rate)
    gain4 = (gain * gain) * (gain * gain)
    mid2 = mid * mid
    push = mid2 * mid * gain4
    ratio = push / top

    begin = None
    for index, (lo, hi) in enumerate(f_groups):
        for copy in forward[index][:-1]:
            copy.wait_recv()
        forward[index][-1].wait()
        block = jnp.concatenate(
            [rbuf[:, p].reshape(size, LANES) for p in range(lo, hi)], axis=1)
        spectra = jnp.dot(half_ref[...], block, preferred_element_type=F32)
        for q, p in enumerate(range(lo, hi)):
            window = slice(q * LANES, (q + 1) * LANES)
            one, two = swap(low, spectra[:inner, window], spectra[inner:, window])
            if p == pairs:
                begin = one
                path[0] = one
            else:
                src[p] = gain * one
                src[pairs + p] = gain * two

    for i in range(COARSE_FACTOR):
        total = src[FINE_FACTOR * i]
        for j in range(1, FINE_FACTOR):
            total = gain * total + src[FINE_FACTOR * i + j]
        tbuf[i] = total
    begin = path[0]

    vref[0] = jnp.where(first, begin, 0.0)
    for i in range(1, COARSE_FACTOR + 1):
        vref[i] = jnp.zeros_like(begin)

    sent = []

    def along(source, target, slot, distance):
        copy = pltpu.make_async_remote_copy(
            src_ref=source, dst_ref=target,
            send_sem=t_send.at[slot], recv_sem=t_recv.at[slot],
            device_id={"tm": tm + distance}, device_id_type=MESH)
        sent.append((copy, distance))

        @pl.when(tm + distance < n_tm)
        def _():
            copy.start()
        return copy

    last = COARSE_FACTOR - 1
    shift = along(tbuf.at[last], lrx, 0, 1)
    drift = gain4 - mid
    slope = 3.0 * gain4 * mid2 * drift + ratio * (push - top)
    aref[...] = begin

    @pl.when(tm >= 1)
    def _():
        shift.wait_recv()
        aref[...] = lrx[...]

    arrived = aref[...]
    ubuf[0] = tbuf[0] + jnp.where(first, gain4 * begin, 0.0)
    bare = jnp.where(first, 0.0, gain4 * arrived)
    base = tbuf[0] + gain4 * arrived
    local = jnp.zeros_like(begin)
    for i in range(1, last):
        relaxed = ubuf[0] if i == 1 else tbuf[i - 1]
        bare = mid * bare + gain4 * relaxed
        local = mid * local + gain4 * (gain4 * base - bare)
        base = tbuf[i] + bare
        ubuf[i] = tbuf[i]
    ubuf[last] = tbuf[last]
    rhs = mid * bare + gain4 * tbuf[last - 1]
    change = gain4 * base - rhs
    zbuf[0, 0] = rhs
    zbuf[0, 1] = local + ratio * change
    near = along(zbuf.at[0], grx.at[0], 1, 1)
    far = along(zbuf.at[0], grx.at[1], 2, 2)
    gbuf[...] = change + (1.0 - ratio) * rhs
    zbuf[1] = jnp.zeros((2,) + begin.shape, F32)

    @pl.when(tm >= 1)
    def _():
        near.wait_recv()
        zbuf[1] = grx[0]

    @pl.when(tm >= 2)
    def _():
        far.wait_recv()
        zbuf[1, 0] = zbuf[1, 0] + top * grx[1, 0]
        zbuf[1, 1] = zbuf[1, 1] + top * grx[1, 1] + slope * grx[1, 0]
    slope = 2.0 * top * slope
    power = top * top
    if not rounds:
        step_in = along(gbuf, wrx, 3, 1)
    for r, d in enumerate(rounds):
        copy = along(zbuf.at[r + 1], zrx.at[r], 4 + r, d)
        if r == 0:
            step_in = along(gbuf, wrx, 3, 1)
        zbuf[r + 2] = zbuf[r + 1]

        @pl.when(tm >= d)
        def _():
            copy.wait_recv()
            zbuf[r + 2, 0] = zbuf[r + 2, 0] + power * zrx[r, 0]
            zbuf[r + 2, 1] = zbuf[r + 2, 1] + power * zrx[r, 1] + slope * zrx[r, 0]
        slope = 2.0 * power * slope
        power = power * power
    aref[...] = jnp.zeros_like(begin)

    @pl.when(tm >= 1)
    def _():
        step_in.wait_recv()
        aref[...] = wrx[...] - (1.0 - ratio) * zbuf[len(rounds) + 1, 0]

    for it in range(ITERS):
        before = vref[0]
        if it == 0:
            incoming = zbuf[len(rounds) + 1, 0]
            ahead = jnp.where(first, 0.0, arrived)
        else:
            ahead = aref[...]
            incoming = zbuf[len(rounds) + 1, 1] - ratio * ahead
            arrived = before + ahead
            for i in range(COARSE_FACTOR):
                ubuf[i] = gain4 * vref[i] + tbuf[i]
        keep = incoming
        for i in range(COARSE_FACTOR):
            if i == 0:
                res = gain4 * ahead
                run = res
            else:
                res = gain4 * (ubuf[i - 1] - vref_old)
                run = mid * run + res
            vref_old = vref[i + 1]
            if i < COARSE_FACTOR - 1:
                keep = mid * keep + res
            else:
                keep = top * incoming + run
            value = ubuf[i] + keep
            vref[i + 1] = value
            for kind, item in enumerate((res, keep, value)):
                at = (kind * ITERS + it) * COARSE_FACTOR + i
                stats[at:at + 1] = jnp.sum(item * item, axis=0, keepdims=True)
        vref[0] = arrived + incoming

    tallies = []
    for k in range(1, n_sp):
        copy = pltpu.make_async_remote_copy(
            src_ref=stats, dst_ref=srx.at[sp], send_sem=q_send.at[k], recv_sem=q_recv.at[k],
            device_id={"space": peers[k]}, device_id_type=MESH)
        copy.start()
        tallies.append(copy)

    for i in range(COARSE_FACTOR):
        current = vref[i]
        for j in range(FINE_FACTOR - 1):
            current = gain * current + src[FINE_FACTOR * i + j]
            path[FINE_FACTOR * i + j] = current
        path[FINE_FACTOR * i + FINE_FACTOR - 1] = vref[i + 1]

    for copies in forward:
        for copy in copies[:-1]:
            copy.wait_send()
    backward = []
    for index, (lo, hi) in enumerate(groups):
        columns = []
        for p in range(lo, hi):
            upper, lower = swap(low, path[p], path[pairs + p])
            columns.append(jnp.concatenate([upper, lower], axis=0))
        block = jnp.concatenate(columns, axis=1)
        high = block.astype(BF16)
        rest = (block - high.astype(F32)).astype(BF16)
        back = jnp.dot(low_ref[...], high, preferred_element_type=F32)
        back = back + jnp.dot(half_ref[...], rest, preferred_element_type=F32)
        back = back + jnp.dot(half_ref[...], high, preferred_element_type=F32)
        back = back.astype(BF16)
        for j in range(n_sp):
            for q, p in enumerate(range(lo, hi)):
                bsend_block = back[j * rows:(j + 1) * rows, q * LANES:(q + 1) * LANES]
                sbuf[j, pairs + 1 + p] = bsend_block
        copies = exchange(sbuf, rbuf, pairs + 1 + lo, pairs + 1 + hi, index, b_send, b_recv, b_local)
        for copy in copies:
            copy.start()
        backward.append(copies)

    for index, (lo, hi) in enumerate(groups):
        for copy in backward[index][:-1]:
            copy.wait_recv()
        backward[index][-1].wait()
        out_ref[:, lo:hi] = rbuf[:, pairs + 1 + lo:pairs + 1 + hi]

    total = stats[...]
    for k in range(1, n_sp):
        tallies[k - 1].wait_recv()
        total = total + srx[lax.rem(sp - k + n_sp, n_sp)]
    total_ref[...] = total

    for copies in backward:
        for copy in copies[:-1]:
            copy.wait_send()
    for copy in tallies:
        copy.wait_send()
    for copy, distance in sent:
        @pl.when(tm + distance < n_tm)
        def _():
            copy.wait_send()


def finish(rows_ref, back_ref, total_ref, out_ref, hist_ref, chg_ref):
    slabs, pairs, rows, _ = rows_ref.shape
    size = out_ref.shape[-1]
    block = jnp.concatenate(
        [rows_ref[j].reshape(pairs * rows, LANES) for j in range(slabs)], axis=1)
    heat = jnp.dot(block, back_ref[...], preferred_element_type=F32)
    for part in range(2):
        out_ref[part] = heat[:, part * size:(part + 1) * size].reshape(pairs, rows, size)
    total = jnp.sum(total_ref[...], axis=1, keepdims=True)
    points = ITERS * COARSE_FACTOR
    residual_norm = jnp.sqrt(total[:points] / (size * size))
    relative = jnp.sqrt(total[points:2 * points] / total[2 * points:3 * points])
    shape = (ITERS, COARSE_FACTOR)
    where = (lax.broadcasted_iota(jnp.int32, shape, 0) * COARSE_FACTOR
             + lax.broadcasted_iota(jnp.int32, shape, 1))
    hist = jnp.zeros(shape, F32)
    chg = jnp.zeros(shape, F32)
    for k in range(points):
        hist = jnp.where(where == k, residual_norm[k:k + 1], hist)
        chg = jnp.where(where == k, relative[k:k + 1], chg)
    hist_ref[...] = hist
    chg_ref[...] = chg


def shards(forcing, starting_heat):
    steps, rows, size = forcing.shape
    n_tm, n_sp = lax.axis_size("tm"), lax.axis_size("space")
    assert steps == FINE_FACTOR * COARSE_FACTOR and 2 * rows == LANES
    pairs = steps // 2
    rounds = []
    reach = 2
    while reach < n_tm - 1:
        rounds.append(reach)
        reach *= 2
    half, low, back, rate = tables(size, n_sp)
    state = (size // 2, LANES)
    slots = len(rounds) + 1
    chunks = pairs // 2 + 1
    stat_rows = 3 * ITERS * COARSE_FACTOR
    dma = pltpu.SemaphoreType.DMA
    vmem = pl.BlockSpec(memory_space=pltpu.VMEM)
    returned, total = pl.pallas_call(
        functools.partial(kernel, n_tm, n_sp, tuple(rounds)),
        out_shape=(
            jax.ShapeDtypeStruct((n_sp, pairs, rows, LANES), BF16),
            jax.ShapeDtypeStruct((stat_rows, LANES), F32),
        ),
        in_specs=[vmem] * 5,
        out_specs=(vmem,) * 2,
        scratch_shapes=[
            pltpu.VMEM((n_sp, 2 * pairs + 1, rows, LANES), BF16),
            pltpu.VMEM((n_sp, 2 * pairs + 1, rows, LANES), BF16),
            pltpu.VMEM((steps,) + state, F32),
            pltpu.VMEM((steps,) + state, F32),
            pltpu.VMEM((COARSE_FACTOR,) + state, F32),
            pltpu.VMEM((COARSE_FACTOR,) + state, F32),
            pltpu.VMEM(state, F32),
            pltpu.VMEM((slots + 1, ITERS) + state, F32),
            pltpu.VMEM(state, F32),
            pltpu.VMEM(state, F32),
            pltpu.VMEM((2, ITERS) + state, F32),
            pltpu.VMEM((slots, ITERS) + state, F32),
            pltpu.VMEM((COARSE_FACTOR + 1,) + state, F32),
            pltpu.VMEM(state, F32),
            pltpu.VMEM((stat_rows, LANES), F32),
            pltpu.VMEM((n_sp, stat_rows, LANES), F32),
            dma((chunks, n_sp)), dma((chunks, n_sp)), dma((chunks,)),
            dma((chunks, n_sp)), dma((chunks, n_sp)), dma((chunks,)),
            dma((4 + len(rounds),)), dma((4 + len(rounds),)),
            dma((n_sp,)), dma((n_sp,)),
        ],
        compiler_params=pltpu.CompilerParams(collective_id=0, has_side_effects=True),
    )(forcing, starting_heat, jnp.asarray(half), jnp.asarray(low), jnp.asarray(rate))
    small = jax.ShapeDtypeStruct((ITERS, COARSE_FACTOR), F32)
    heat, history, change = pl.pallas_call(
        finish,
        grid=(pairs // 2,),
        out_shape=(jax.ShapeDtypeStruct((2, pairs, rows, size), F32), small, small),
        in_specs=[
            pl.BlockSpec((n_sp, 2, rows, LANES), lambda p: (0, p, 0, 0)),
            pl.BlockSpec((2 * size, 2 * size), lambda p: (0, 0)),
            pl.BlockSpec((stat_rows, LANES), lambda p: (0, 0)),
        ],
        out_specs=(
            pl.BlockSpec((2, 2, rows, size), lambda p: (0, p, 0, 0)),
            pl.BlockSpec(small.shape, lambda p: (0, 0)),
            pl.BlockSpec(small.shape, lambda p: (0, 0)),
        ),
    )(returned, jnp.asarray(back), total)
    return heat.reshape(steps, rows, size), history, change


def solution(mesh):
    return jax.shard_map(
        shards,
        mesh=mesh,
        in_specs=(P("tm", "space", None), P("space", None)),
        out_specs=(P("tm", "space", None), P(None, "tm"), P(None, "tm")),
        check_vma=False,
    )
```

```python
import functools
import math

import jax
import jax.numpy as jnp
import numpy as np
from jax import lax
from jax.experimental import pallas as pl
from jax.experimental.pallas import tpu as pltpu
from jax.sharding import PartitionSpec as P

FINE_FACTOR = 4
COARSE_FACTOR = 4
ITERS = 2
DURATION = 0.004
LANES = 128
MESH = pl.DeviceIdType.MESH
F32 = jnp.float32
BF16 = jnp.bfloat16


def sine_table(size):
    numbers = np.arange(1, size + 1, dtype=np.int64)
    product = numbers[:, None] * numbers[None, :] % (2 * (size + 1))
    return (math.sqrt(2.0 / (size + 1)) * np.sin(np.pi * product / (size + 1))).astype(np.float32)


def eigenvalues(size):
    numbers = np.arange(1, size + 1, dtype=np.float64)
    return 4.0 * (size + 1) ** 2 * np.sin(np.pi * numbers / (2 * (size + 1))) ** 2


def tables(size, slabs):
    width = size // slabs
    full = sine_table(size)
    half = full.astype(BF16)
    low = (full - half.astype(np.float32)).astype(BF16)
    back = np.zeros((slabs, 2, width, 2, size), BF16)
    for part in range(2):
        back[:, part, :, part, :] = half.reshape(slabs, width, size)
    back = back.reshape(2 * size, 2 * size)
    mu = eigenvalues(size)
    rate = mu.reshape(1, 2, size // 2, 1) + mu.reshape(slabs, 1, 1, width)
    rate = rate.transpose(0, 2, 1, 3).reshape(slabs, size // 2, 2 * width).astype(np.float32)
    return half, low, back, rate


def swap(low, a, b):
    half = LANES // 2
    return (
        jnp.where(low, a, pltpu.roll(b, half, 1)),
        jnp.where(low, pltpu.roll(a, half, 1), b),
    )


def kernel(n_tm, n_sp, rounds, f_ref, s_ref, half_ref, low_ref, rate_ref,
           out_ref, total_ref,
           sbuf, rbuf, src, path, tbuf, ubuf, lbuf, gbuf, zbuf, lrx, grx, zrx, vref, aref, stats, srx,
           f_send, f_recv, f_local, b_send, b_recv, b_local, t_send, t_recv, q_send, q_recv):
    tm, sp = lax.axis_index("tm"), lax.axis_index("space")
    steps, rows, size = f_ref.shape
    pairs = steps // 2
    inner = size // 2
    first = tm == 0
    distances = [1, 2] + [d for d in rounds if d > 2]
    peers = [lax.rem(sp + k, n_sp) for k in range(n_sp)]
    low = lax.broadcasted_iota(jnp.int32, (1, LANES), 1) < LANES // 2

    barrier = pltpu.get_barrier_semaphore()
    count = n_sp - 1
    for k in range(1, n_sp):
        pl.semaphore_signal(barrier, inc=1, device_id={"space": peers[k]}, device_id_type=MESH)
    for d in distances:
        @pl.when(tm + d < n_tm)
        def _():
            pl.semaphore_signal(barrier, inc=1, device_id={"tm": tm + d}, device_id_type=MESH)

        @pl.when(tm >= d)
        def _():
            pl.semaphore_signal(barrier, inc=1, device_id={"tm": tm - d}, device_id_type=MESH)
        count = count + (tm + d < n_tm).astype(jnp.int32) + (tm >= d).astype(jnp.int32)

    groups = [(p, p + 2) for p in range(0, pairs, 2)]
    groups[0] = (0, 2)
    f_groups = [(pairs, pairs + 1)] + groups

    def exchange(source, target, lo, hi, index, send, recv, local):
        copies = []
        for k in range(1, n_sp):
            copies.append(pltpu.make_async_remote_copy(
                src_ref=source.at[peers[k], pl.ds(lo, hi - lo)],
                dst_ref=target.at[sp, pl.ds(lo, hi - lo)],
                send_sem=send.at[index, k], recv_sem=recv.at[index, k],
                device_id={"space": peers[k]}, device_id_type=MESH))
        copies.append(pltpu.make_async_copy(
            source.at[sp, pl.ds(lo, hi - lo)], target.at[sp, pl.ds(lo, hi - lo)], local.at[index]))
        return copies

    forward = []
    for index, (lo, hi) in enumerate(f_groups):
        if lo == pairs:
            a = jnp.dot(s_ref[...], half_ref[...], preferred_element_type=F32)
            b = a
        else:
            a = jnp.dot(f_ref[lo:hi].reshape((hi - lo) * rows, size), half_ref[...],
                        preferred_element_type=F32)
            b = jnp.dot(f_ref[pairs + lo:pairs + hi].reshape((hi - lo) * rows, size), half_ref[...],
                        preferred_element_type=F32)
        for g in range(size // LANES):
            window = slice(g * LANES, (g + 1) * LANES)
            even, odd = swap(low, a[:, window], b[:, window])
            sbuf[2 * g, lo:hi] = even.astype(BF16).reshape(hi - lo, rows, LANES)
            sbuf[2 * g + 1, lo:hi] = odd.astype(BF16).reshape(hi - lo, rows, LANES)
        if index == 0:
            pl.semaphore_wait(barrier, count)
        copies = exchange(sbuf, rbuf, lo, hi, index, f_send, f_recv, f_local)
        for copy in copies:
            copy.start()
        forward.append(copies)

    step = DURATION / (steps * n_tm)
    rate = rate_ref[sp]
    gain = 1.0 / (1.0 + step * rate)
    mid = 1.0 / (1.0 + FINE_FACTOR * step * rate)
    top = 1.0 / (1.0 + FINE_FACTOR * COARSE_FACTOR * step * rate)
    gain4 = (gain * gain) * (gain * gain)
    mid2 = mid * mid
    push = mid2 * mid * gain4
    ratio = push / top

    begin = None
    for index, (lo, hi) in enumerate(f_groups):
        for copy in forward[index][:-1]:
            copy.wait_recv()
        forward[index][-1].wait()
        block = jnp.concatenate(
            [rbuf[:, p].reshape(size, LANES) for p in range(lo, hi)], axis=1)
        spectra = jnp.dot(half_ref[...], block, preferred_element_type=F32)
        for q, p in enumerate(range(lo, hi)):
            window = slice(q * LANES, (q + 1) * LANES)
            one, two = swap(low, spectra[:inner, window], spectra[inner:, window])
            if p == pairs:
                begin = one
                path[0] = one
            else:
                src[p] = gain * one
                src[pairs + p] = gain * two

    for i in range(COARSE_FACTOR):
        total = src[FINE_FACTOR * i]
        for j in range(1, FINE_FACTOR):
            total = gain * total + src[FINE_FACTOR * i + j]
        tbuf[i] = total
    begin = path[0]

    vref[0] = jnp.where(first, begin, 0.0)
    for i in range(1, COARSE_FACTOR + 1):
        vref[i] = jnp.zeros_like(begin)

    sent = []

    def along(source, target, slot, it, distance):
        copy = pltpu.make_async_remote_copy(
            src_ref=source, dst_ref=target,
            send_sem=t_send.at[it, slot], recv_sem=t_recv.at[it, slot],
            device_id={"tm": tm + distance}, device_id_type=MESH)
        sent.append((copy, distance))

        @pl.when(tm + distance < n_tm)
        def _():
            copy.start()
        return copy

    for it in range(ITERS):
        last = COARSE_FACTOR - 1
        newest = gain4 * vref[last] + tbuf[last]
        lbuf[it] = newest
        shift = along(lbuf.at[it], lrx.at[it], 0, it, 1)
        relaxed = [gain4 * vref[i] + tbuf[i] for i in range(last)] + [newest]
        residual = [None] + [gain4 * (relaxed[i - 1] - vref[i]) for i in range(1, COARSE_FACTOR)]
        local = residual[1]
        for i in range(2, COARSE_FACTOR):
            local = mid * local + residual[i]
        gbuf[it] = local - jnp.where(first, 0.0, push * vref[0]) + ratio * newest
        near = along(gbuf.at[it], grx.at[it, 0], 1, it, 1)
        far = along(gbuf.at[it], grx.at[it, 1], 2, it, 2)
        for i in range(COARSE_FACTOR):
            ubuf[i] = relaxed[i]
        zbuf[it, 0] = jnp.zeros_like(begin)
        aref[...] = begin

        @pl.when(tm >= 1)
        def _():
            shift.wait_recv()
            aref[...] = lrx[it]
            near.wait_recv()
            zbuf[it, 0] = grx[it, 0]

        @pl.when(tm >= 2)
        def _():
            far.wait_recv()
            zbuf[it, 0] = zbuf[it, 0] + top * grx[it, 1]
        power = top * top
        for r, d in enumerate(rounds):
            copy = along(zbuf.at[it, r], zrx.at[it, r], 3 + r, it, d)
            zbuf[it, r + 1] = zbuf[it, r]

            @pl.when(tm >= d)
            def _():
                copy.wait_recv()
                zbuf[it, r + 1] = zbuf[it, r + 1] + power * zrx[it, r]
            power = power * power
        arrived = aref[...]
        incoming = jnp.where(first, 0.0, zbuf[it, len(rounds)] - ratio * arrived)
        before = vref[0]
        keep = incoming
        for i in range(COARSE_FACTOR):
            if i == 0:
                res = gain4 * (arrived - before)
                run = res
            else:
                res = gain4 * (ubuf[i - 1] - vref_old)
                run = mid * run + res
            vref_old = vref[i + 1]
            if i < COARSE_FACTOR - 1:
                keep = mid * keep + res
            else:
                keep = top * incoming + run
            value = ubuf[i] + keep
            vref[i + 1] = value
            for kind, item in enumerate((res, keep, value)):
                at = (kind * ITERS + it) * COARSE_FACTOR + i
                stats[at:at + 1] = jnp.sum(item * item, axis=0, keepdims=True)
        vref[0] = arrived + incoming

    tallies = []
    for k in range(1, n_sp):
        copy = pltpu.make_async_remote_copy(
            src_ref=stats, dst_ref=srx.at[sp], send_sem=q_send.at[k], recv_sem=q_recv.at[k],
            device_id={"space": peers[k]}, device_id_type=MESH)
        copy.start()
        tallies.append(copy)

    for i in range(COARSE_FACTOR):
        current = vref[i]
        for j in range(FINE_FACTOR - 1):
            current = gain * current + src[FINE_FACTOR * i + j]
            path[FINE_FACTOR * i + j] = current
        path[FINE_FACTOR * i + FINE_FACTOR - 1] = vref[i + 1]

    for copies in forward:
        for copy in copies[:-1]:
            copy.wait_send()
    backward = []
    for index, (lo, hi) in enumerate(groups):
        columns = []
        for p in range(lo, hi):
            upper, lower = swap(low, path[p], path[pairs + p])
            columns.append(jnp.concatenate([upper, lower], axis=0))
        block = jnp.concatenate(columns, axis=1)
        high = block.astype(BF16)
        rest = (block - high.astype(F32)).astype(BF16)
        back = jnp.dot(low_ref[...], high, preferred_element_type=F32)
        back = back + jnp.dot(half_ref[...], rest, preferred_element_type=F32)
        back = back + jnp.dot(half_ref[...], high, preferred_element_type=F32)
        back = back.astype(BF16)
        for j in range(n_sp):
            for q, p in enumerate(range(lo, hi)):
                bsend_block = back[j * rows:(j + 1) * rows, q * LANES:(q + 1) * LANES]
                sbuf[j, pairs + 1 + p] = bsend_block
        copies = exchange(sbuf, rbuf, pairs + 1 + lo, pairs + 1 + hi, index, b_send, b_recv, b_local)
        for copy in copies:
            copy.start()
        backward.append(copies)

    for index, (lo, hi) in enumerate(groups):
        for copy in backward[index][:-1]:
            copy.wait_recv()
        backward[index][-1].wait()
        out_ref[:, lo:hi] = rbuf[:, pairs + 1 + lo:pairs + 1 + hi]

    total = stats[...]
    for k in range(1, n_sp):
        tallies[k - 1].wait_recv()
        total = total + srx[lax.rem(sp - k + n_sp, n_sp)]
    total_ref[...] = total

    for copies in backward:
        for copy in copies[:-1]:
            copy.wait_send()
    for copy in tallies:
        copy.wait_send()
    for copy, distance in sent:
        @pl.when(tm + distance < n_tm)
        def _():
            copy.wait_send()


def finish(rows_ref, back_ref, total_ref, out_ref, hist_ref, chg_ref):
    slabs, pairs, rows, _ = rows_ref.shape
    size = out_ref.shape[-1]
    block = jnp.concatenate(
        [rows_ref[j].reshape(pairs * rows, LANES) for j in range(slabs)], axis=1)
    heat = jnp.dot(block, back_ref[...], preferred_element_type=F32)
    for part in range(2):
        out_ref[part] = heat[:, part * size:(part + 1) * size].reshape(pairs, rows, size)
    total = jnp.sum(total_ref[...], axis=1, keepdims=True)
    points = ITERS * COARSE_FACTOR
    residual_norm = jnp.sqrt(total[:points] / (size * size))
    relative = jnp.sqrt(total[points:2 * points] / total[2 * points:3 * points])
    shape = (ITERS, COARSE_FACTOR)
    where = (lax.broadcasted_iota(jnp.int32, shape, 0) * COARSE_FACTOR
             + lax.broadcasted_iota(jnp.int32, shape, 1))
    hist = jnp.zeros(shape, F32)
    chg = jnp.zeros(shape, F32)
    for k in range(points):
        hist = jnp.where(where == k, residual_norm[k:k + 1], hist)
        chg = jnp.where(where == k, relative[k:k + 1], chg)
    hist_ref[...] = hist
    chg_ref[...] = chg


def shards(forcing, starting_heat):
    steps, rows, size = forcing.shape
    n_tm, n_sp = lax.axis_size("tm"), lax.axis_size("space")
    assert steps == FINE_FACTOR * COARSE_FACTOR and 2 * rows == LANES
    pairs = steps // 2
    rounds = []
    reach = 2
    while reach < n_tm - 1:
        rounds.append(reach)
        reach *= 2
    half, low, back, rate = tables(size, n_sp)
    state = (size // 2, LANES)
    slots = len(rounds) + 1
    chunks = pairs // 2 + 1
    stat_rows = 3 * ITERS * COARSE_FACTOR
    dma = pltpu.SemaphoreType.DMA
    vmem = pl.BlockSpec(memory_space=pltpu.VMEM)
    returned, total = pl.pallas_call(
        functools.partial(kernel, n_tm, n_sp, tuple(rounds)),
        out_shape=(
            jax.ShapeDtypeStruct((n_sp, pairs, rows, LANES), BF16),
            jax.ShapeDtypeStruct((stat_rows, LANES), F32),
        ),
        in_specs=[vmem] * 5,
        out_specs=(vmem,) * 2,
        scratch_shapes=[
            pltpu.VMEM((n_sp, 2 * pairs + 1, rows, LANES), BF16),
            pltpu.VMEM((n_sp, 2 * pairs + 1, rows, LANES), BF16),
            pltpu.VMEM((steps,) + state, F32),
            pltpu.VMEM((steps,) + state, F32),
            pltpu.VMEM((COARSE_FACTOR,) + state, F32),
            pltpu.VMEM((COARSE_FACTOR,) + state, F32),
            pltpu.VMEM((ITERS,) + state, F32),
            pltpu.VMEM((ITERS,) + state, F32),
            pltpu.VMEM((ITERS, slots) + state, F32),
            pltpu.VMEM((ITERS,) + state, F32),
            pltpu.VMEM((ITERS, 2) + state, F32),
            pltpu.VMEM((ITERS, slots) + state, F32),
            pltpu.VMEM((COARSE_FACTOR + 1,) + state, F32),
            pltpu.VMEM(state, F32),
            pltpu.VMEM((stat_rows, LANES), F32),
            pltpu.VMEM((n_sp, stat_rows, LANES), F32),
            dma((chunks, n_sp)), dma((chunks, n_sp)), dma((chunks,)),
            dma((chunks, n_sp)), dma((chunks, n_sp)), dma((chunks,)),
            dma((ITERS, 3 + len(rounds))), dma((ITERS, 3 + len(rounds))),
            dma((n_sp,)), dma((n_sp,)),
        ],
        compiler_params=pltpu.CompilerParams(collective_id=0, has_side_effects=True),
    )(forcing, starting_heat, jnp.asarray(half), jnp.asarray(low), jnp.asarray(rate))
    small = jax.ShapeDtypeStruct((ITERS, COARSE_FACTOR), F32)
    heat, history, change = pl.pallas_call(
        finish,
        grid=(pairs // 2,),
        out_shape=(jax.ShapeDtypeStruct((2, pairs, rows, size), F32), small, small),
        in_specs=[
            pl.BlockSpec((n_sp, 2, rows, LANES), lambda p: (0, p, 0, 0)),
            pl.BlockSpec((2 * size, 2 * size), lambda p: (0, 0)),
            pl.BlockSpec((stat_rows, LANES), lambda p: (0, 0)),
        ],
        out_specs=(
            pl.BlockSpec((2, 2, rows, size), lambda p: (0, p, 0, 0)),
            pl.BlockSpec(small.shape, lambda p: (0, 0)),
            pl.BlockSpec(small.shape, lambda p: (0, 0)),
        ),
    )(returned, jnp.asarray(back), total)
    return heat.reshape(steps, rows, size), history, change


def solution(mesh):
    return jax.shard_map(
        shards,
        mesh=mesh,
        in_specs=(P("tm", "space", None), P("space", None)),
        out_specs=(P("tm", "space", None), P(None, "tm"), P(None, "tm")),
        check_vma=False,
    )
```
